32 devices in a mesh: tm: 8 (over z, y), obs: 4 (over x, core).
Axes of the slice: x: 2, y: 2, z: 4, core: 2. Of those that a mesh axis runs over, the one named last changes fastest.
Arguments:
- trajectory: bfloat16 [8, 64, 256, 128], P('tm', 'obs'), may hold values from -6 to 6
- weights: bfloat16 [1024, 128, 256], P(('tm', 'obs')), may hold values from -0.375 to 0.375
- observed: bfloat16 [1024, 128, 128], P(('tm', 'obs')), may hold values from -9 to 9
- window: int32 [1024, 1], P(('tm', 'obs')), may hold values from 0 to 7; in each aligned block of 32 rows (0 to 31, 32 to 63, ...) at most 4 rows name the same one
- block: int32 [1024], P(('tm', 'obs')), may hold values from 0 to 15
- counts: int32 [1024], P(('tm', 'obs')), may hold values from 32 to 128, as said below
- flags: int32 [1024, 128], P(('tm', 'obs')), may hold values 0 or 1
- inv_error: float32 [128], replicated, may hold values from 0.5 to 2
Outputs:
- departures: bfloat16 [1024, 128, 128], P(('tm', 'obs'))
- window_bias: float32 [8, 128], P('tm')
- window_chi: float32 [8, 128], P('tm')
The draws below stay inside these ranges and needn't reach their ends.
Inputs may be any that keep to these rules, and one draw needn't show every extreme that they name: Among the 32 groups of one device, no sub-window is named by more than 4. `counts`: among the 32 groups of one device, one has all 128 slots live.
All inputs are finite; a program needn't handle non-finite values. No bound on the sum of `flags` on one device may be relied on, other than what follows from the above.
Results may differ from the reference program's by a relative error of at most 0.001.
Values may be sent and summed in bfloat16 or wider, within the bound.
No kernel may reach another device: no remote copies, remote signals or barrier semaphores. Data moves between devices by JAX's collectives and lax.ppermute only.
A program may use at most 64 MiB of HBM per device.

```python
import math
import jax
import jax.numpy as jnp
import numpy as np
from jax import lax

LEV = 128
G = 256
BL = 16
CAPB = 128
NGRP = 32
GCAP = 4
NT = 8
NB = 64
NGRP_ALL = 1024
N_TM = 8
N_OBS = 4


def draw_counts(key, part):
    devices = N_TM * N_OBS
    first_key = jax.random.fold_in(key, 11)
    second_key = jax.random.fold_in(key, 23)
    values = jax.random.randint(first_key, (devices, NGRP), CAPB // 4, CAPB + 1)
    full_at = jax.random.randint(second_key, (devices,), 0, NGRP)
    column = jnp.arange(NGRP, dtype=jnp.int32)[None, :]
    values = jnp.where(column == full_at[:, None], CAPB, values)
    return values.reshape(devices * NGRP).astype(jnp.int32)


def place_ends(array, rng, least, high):
    place = [jax.random.randint(jax.random.fold_in(rng, axis), (), 0, length) for axis, length in enumerate(array.shape)]
    widest = array.shape.index(max(array.shape))
    neighbour = place[:widest] + [(place[widest] + 1) % array.shape[widest]] + place[widest + 1:]
    return array.at[tuple(place)].set(least).at[tuple(neighbour)].set(high)


def block_scale(own_key, shape, pieces, low, largest):
    loudness, own = 1.0, jax.random.fold_in(own_key, 6)
    for position, shards_of in pieces:
        steps = jnp.exp(jax.random.uniform(jax.random.fold_in(own, position), (shards_of,), jnp.float32, low / len(pieces), largest / len(pieces)))
        loudness = loudness * jnp.repeat(steps, shape[position] // shards_of).reshape([-1 if axis == position else 1 for axis in range(len(shape))])
    return loudness


def shared_out(stream_key, own, number, rows, number_of, top, bound, lean):
    ranking = jax.random.permutation(stream_key, number_of)
    packed, usual = load_shares(number_of, rows * top, bound, lean, True), load_shares(number_of, rows * top, bound, lean, False)
    places = jnp.arange(number_of)

    def named(sizes, turn):
        used = int((sizes > 0).sum())
        fixed = max(1, used // 4)
        shifted = fixed + (places - fixed + turn * (used - fixed)) % max(1, number_of - fixed)
        return jnp.zeros((number_of,), jnp.int32).at[ranking[jnp.where(places < fixed, places, shifted)]].set(jnp.asarray(sizes, jnp.int32))

    sizes = jnp.where(number % 4 == 0, named(packed, number // 4), named(usual, number - number // 4 - 1))
    mixed = jax.random.permutation(jax.random.fold_in(own, 3), number_of)
    source_of, sink = mixed[0:number_of // 2 * 2:2], mixed[1:number_of // 2 * 2:2]
    margin = jnp.minimum(sizes[source_of] - 1, bound - sizes[sink]) // 2
    margin = jnp.where((source_of == ranking[0]) | (sink == ranking[0]) | (sizes[sink] == 0), 0, jnp.maximum(margin, 0))
    shifted = jax.random.randint(jax.random.fold_in(own, 4), (number_of // 2,), 0, 1 << 20) % (margin + 1)
    sizes = sizes.at[source_of].add(-shifted).at[sink].add(shifted)
    items = jnp.searchsorted(jnp.cumsum(sizes), jnp.arange(rows * top), side="right").astype(jnp.int32)
    table = items.reshape(top, rows).T
    table = table[jax.random.permutation(jax.random.fold_in(own, 1), rows)]
    turn = jax.random.randint(jax.random.fold_in(own, 2), (rows, 1), 0, top)
    return jnp.take_along_axis(table, (jnp.arange(top)[None, :] + turn) % top, axis=1)


def load_shares(count, total, bound, lean, full):
    loads = [(1 << 20) // math.isqrt(rank ** lean) + 1 for rank in range(1, count + 1)]
    largest = bound if full else min(bound, max(-(-total // count), total * loads[0] // sum(loads)))
    least = 1 if total - largest >= count - 1 else 0
    given, surplus = [largest] + [least] * (count - 1), total - largest - least * (count - 1)
    while surplus > 0:
        candidates = [i for i in range(1, count) if given[i] < largest] or [i for i in range(1, count) if given[i] < bound]
        mass, remaining = sum([loads[i] for i in candidates]), surplus
        for i in candidates:
            extra = min(bound - given[i], max(1, remaining * loads[i] // mass), surplus)
            given[i] = given[i] + extra
            surplus = surplus - extra
    return np.array(given)


def bell_draw(rng, shape, deviation, most, shards=(), kind=jnp.bfloat16):
    entries = jax.random.normal(rng, shape, jnp.float32) * deviation
    if len(shards) > 0:
        entries = block_scale(rng, shape, shards, -0.22, 0.18) * entries
    return jnp.clip(entries, min=-most, max=most).astype(kind)


def setup_inputs(seed: int = 0) -> dict:
    keys = jax.random.split(jax.random.key(seed), 9)
    trajectory = bell_draw(keys[0], (NT, NB, G, LEV), 1.0, 6.0, ((0, 8), (1, 4)))
    weights = bell_draw(keys[1], (NGRP_ALL, CAPB, G), G ** -0.5, 0.375, ((0, 32),))
    observed = bell_draw(keys[2], (NGRP_ALL, CAPB, LEV), 1.5, 9.0, ((0, 32),))
    window_keys = jax.random.split(jax.random.fold_in(keys[3], 1), NGRP_ALL // NGRP)
    window_turns = jax.random.permutation(jax.random.fold_in(keys[3], 3), NGRP_ALL // NGRP)
    window = jax.vmap(lambda own, number: shared_out(jax.random.fold_in(keys[3], 2), own, number, NGRP, NT, 1, GCAP, 2))(window_keys, window_turns).reshape((NGRP_ALL, 1))
    block = place_ends(jax.random.randint(keys[4], (NGRP_ALL,), 0, BL), jax.random.fold_in(keys[4], 1), 0, BL - 1).astype(jnp.int32)
    counts = draw_counts(jax.random.fold_in(keys[8], 71), 0)
    flags = place_ends((jax.random.randint(keys[6], (NGRP_ALL, CAPB), 0, 4) < 3).astype(jnp.int32), jax.random.fold_in(keys[6], 1), 0, 1)
    inv_error = jnp.clip(jnp.exp(jax.random.uniform(keys[7], (LEV,), jnp.float32, math.log(0.5), math.log(2.0))), 0.5, 2.0)
    return {"trajectory": trajectory, "weights": weights, "observed": observed, "window": window, "block": block, "counts": counts, "flags": flags, "inv_error": inv_error}


def reference(trajectory, weights, observed, window, block, counts, flags, inv_error):
    devices = N_TM * N_OBS
    nwin = N_TM
    w_dev = weights.reshape(devices, NGRP, CAPB, G)
    y_dev = observed.reshape(devices, NGRP, CAPB, LEV)
    win_dev = window.reshape(devices, NGRP).astype(jnp.int32)
    blk_dev = block.reshape(devices, NGRP).astype(jnp.int32)
    cnt_dev = counts.reshape(devices, NGRP).astype(jnp.int32)
    flg_dev = flags.reshape(devices, NGRP, CAPB).astype(jnp.int32)
    dev_ids = jnp.arange(devices, dtype=jnp.int32)

    def one_device(items):
        dev, w_here, y_here, win_here, blk_here, cnt_here, flg_here = items
        region = (dev % N_OBS).astype(jnp.int32)
        slab = lax.dynamic_slice_in_dim(trajectory, region * BL, BL, 1)
        picked = slab[win_here, blk_here].astype(jnp.float32)
        hx = jnp.einsum('gop,gpl->gol', w_here.astype(jnp.float32), picked)
        slot_ids = jnp.arange(CAPB, dtype=jnp.int32)
        used = jnp.where(slot_ids[None, :] < cnt_here[:, None], flg_here, 0).astype(jnp.float32)
        departure = used[:, :, None] * (y_here.astype(jnp.float32) - hx) * inv_error[None, None, :]
        member = (win_here[:, None] == jnp.arange(nwin, dtype=jnp.int32)[None, :]).astype(jnp.float32)
        sum_one = jnp.einsum('gt,gl->tl', member, lax.optimization_barrier(jnp.sum(departure, 1)), precision=lax.Precision.HIGHEST)
        sum_two = jnp.einsum('gt,gl->tl', member, lax.optimization_barrier(jnp.sum(departure * departure, 1)), precision=lax.Precision.HIGHEST)
        kept = jnp.einsum('gt,g->t', member, lax.optimization_barrier(jnp.sum(used, 1)), precision=lax.Precision.HIGHEST)
        return (departure.astype(jnp.bfloat16), sum_one, sum_two, kept)
    deps, ones, twos, kepts = lax.map(one_device, (dev_ids, w_dev, y_dev, win_dev, blk_dev, cnt_dev, flg_dev))
    sum_one = lax.optimization_barrier(jnp.sum(ones, 0))
    sum_two = lax.optimization_barrier(jnp.sum(twos, 0))
    kept = lax.optimization_barrier(jnp.sum(kepts, 0))
    departures = deps.reshape(NGRP * devices, CAPB, LEV)
    window_bias = sum_one / jnp.sqrt(kept[:, None] + 1.0)
    window_chi = sum_two / (kept[:, None] + 1.0)
    return (departures, window_bias, window_chi)
```

```python
import jax
import jax.numpy as jnp
from jax import lax
from jax.experimental import pallas as pl
from jax.experimental.pallas import tpu as pltpu
from jax.sharding import PartitionSpec as P

GCAP = 4
STEP = 8


ANY = pl.BlockSpec(memory_space=pl.ANY)
SMEM = pl.BlockSpec(memory_space=pltpu.SMEM)


def swap(x, axis, bits):
    size = lax.axis_size(axis)
    return lax.ppermute(x, axis, [(i, i ^ bits) for i in range(size)])


def gather_rows(ids, slab, pieces, first, rows):
    width = slab.shape[2]

    def body(ids_ref, slab_ref, *refs):
        outs, sems = refs[:pieces], refs[pieces]
        copies = []
        for piece in range(pieces):
            for k in range(GCAP):
                copy = pltpu.make_async_copy(
                    slab_ref.at[ids_ref[piece, k], pl.ds(first, rows)],
                    outs[piece].at[k],
                    sems.at[piece * GCAP + k],
                )
                copy.start()
                copies.append(copy)
        for copy in copies:
            copy.wait()

    return pl.pallas_call(
        body,
        in_specs=[SMEM, ANY],
        out_specs=[ANY] * pieces,
        out_shape=[jax.ShapeDtypeStruct((GCAP, rows, width), slab.dtype)] * pieces,
        scratch_shapes=[pltpu.SemaphoreType.DMA((pieces * GCAP,))],
    )(ids, slab)


def departures_kernel(
    slab, mirror, near, far_low, far_high, slot_of, win_of, own_ids, mirror_ids, weights, observed, used_t, inv_error,
    kept_rows, low,
):
    groups, slots, cells = weights.shape
    levels = observed.shape[2]
    windows = kept_rows.shape[0]
    half = windows // 2
    n_near, n_low, n_high = len(near), len(far_low), len(far_high)
    opposite = windows - 2
    n_sems = 2 * GCAP + n_near + n_low + n_high

    def body(slot_ref, win_ref, own_ref, mir_ref, w_ref, y_ref, u_ref, inv_ref, kept_ref, slab_ref, mirror_ref, *refs):
        near_refs = refs[:n_near]
        low_refs = refs[n_near:n_near + n_low]
        high_refs = refs[n_near + n_low:n_near + n_low + n_high]
        out_ref, sum_ref, x_ref, sems = refs[n_near + n_low + n_high:]
        step = pl.program_id(0)

        @pl.when(step == 0)
        def _():
            copies = []

            def add(src, dst):
                copy = pltpu.make_async_copy(src, dst, sems.at[len(copies)])
                copy.start()
                copies.append(copy)

            for k in range(GCAP):
                add(slab_ref.at[own_ref[k]], x_ref.at[k])
                add(mirror_ref.at[mir_ref[k]], x_ref.at[opposite * GCAP + k, pl.ds(0, low)])
            for j in range(1, half):
                add(near_refs[j - 1], x_ref.at[pl.ds(j * GCAP, GCAP)])
                add(low_refs[j - 1], x_ref.at[pl.ds((j ^ opposite) * GCAP, GCAP), pl.ds(0, low)])
            for j in range(half, windows):
                add(high_refs[j - half], x_ref.at[pl.ds(j * GCAP, GCAP), pl.ds(low, cells - low)])
            sum_ref[0] = jnp.zeros((windows, levels), jnp.float32)
            sum_ref[1] = jnp.zeros((windows, levels), jnp.float32)
            sum_ref[2] = kept_ref[...]
            for copy in copies:
                copy.wait()

        inv = inv_ref[...]
        for i in range(STEP):
            g = step * STEP + i
            x = x_ref[slot_ref[g]]
            hx = jnp.dot(w_ref[i], x, preferred_element_type=jnp.float32)
            dep = u_ref[0, :, i:i + 1] * (y_ref[i].astype(jnp.float32) - hx) * inv
            out_ref[i] = dep.astype(jnp.bfloat16)
            w = win_ref[g]
            sum_ref[0, pl.ds(w, 1), :] += jnp.sum(dep, 0, keepdims=True)
            sum_ref[1, pl.ds(w, 1), :] += jnp.sum(dep * dep, 0, keepdims=True)

    return pl.pallas_call(
        body,
        grid=(groups // STEP,),
        in_specs=[SMEM] * 4
        + [
            pl.BlockSpec((STEP, slots, cells), lambda s: (s, 0, 0)),
            pl.BlockSpec((STEP, slots, levels), lambda s: (s, 0, 0)),
            pl.BlockSpec((1, slots, STEP), lambda s: (s, 0, 0)),
            pl.BlockSpec((1, levels), lambda s: (0, 0)),
            pl.BlockSpec((windows, levels), lambda s: (0, 0)),
        ]
        + [ANY] * (2 + n_near + n_low + n_high),
        out_specs=[
            pl.BlockSpec((STEP, slots, levels), lambda s: (s, 0, 0)),
            pl.BlockSpec((3, windows, levels), lambda s: (0, 0, 0)),
        ],
        out_shape=[
            jax.ShapeDtypeStruct((groups, slots, levels), jnp.bfloat16),
            jax.ShapeDtypeStruct((3, windows, levels), jnp.float32),
        ],
        scratch_shapes=[
            pltpu.VMEM((windows * GCAP, cells, levels), slab.dtype),
            pltpu.SemaphoreType.DMA((n_sems,)),
        ],
    )(
        slot_of, win_of, own_ids, mirror_ids, weights, observed, used_t, inv_error[None, :], kept_rows,
        slab, mirror, *near, *far_low, *far_high,
    )


def per_device(trajectory, weights, observed, window, block, counts, flags, inv_error):
    groups, slots, cells = weights.shape
    levels = observed.shape[2]
    windows = lax.axis_size("tm")
    half = windows // 2
    opposite = windows - 2
    low = cells * 3 // 8 // 16 * 16
    me = lax.axis_index("tm")
    slab = trajectory[0]

    mirror = swap(slab[:, :low], "tm", opposite)

    win_of = window[:, 0]
    gid = jnp.arange(groups, dtype=jnp.int32)
    rank = jnp.sum(((win_of[:, None] == win_of[None, :]) & (gid[None, :] < gid[:, None])).astype(jnp.int32), 1)
    code = win_of * GCAP + rank
    wanted = jnp.sum(
        jnp.where(code[None, :] == jnp.arange(windows * GCAP, dtype=jnp.int32)[:, None], block[None, :], 0), 1
    ).reshape(windows, GCAP)
    across = wanted.reshape(2, half // 2, 2, GCAP)[::-1, ::-1].reshape(windows, GCAP)
    request = jnp.concatenate([wanted, across], 1)
    asked = lax.all_to_all(request, "tm", split_axis=0, concat_axis=0, tiled=True)
    by_xor = asked[jnp.arange(windows, dtype=jnp.int32) ^ me]

    send_high = gather_rows(by_xor[half:, :GCAP], slab, half, low, cells - low)
    far_high = [swap(send_high[j - half], "tm", j) for j in range(half, windows)]
    send_near = gather_rows(by_xor[1:half, :GCAP], slab, half - 1, 0, cells)
    near = [swap(send_near[j - 1], "tm", j) for j in range(1, half)]
    send_low = gather_rows(by_xor[1:half, GCAP:], mirror, half - 1, 0, low)
    far_low = [swap(send_low[j - 1], "tm", j) for j in range(1, half)]

    slot_ids = lax.broadcasted_iota(jnp.int32, (groups, slots), 1)
    used = jnp.where(slot_ids < counts[:, None], flags, 0).astype(jnp.float32)
    used_t = used.reshape(groups // STEP, STEP, slots).transpose(0, 2, 1)
    member = win_of[None, :] == jnp.arange(windows, dtype=jnp.int32)[:, None]
    kept = jnp.sum(jnp.where(member, jnp.sum(used, 1)[None, :], 0.0), 1)
    kept_rows = jnp.broadcast_to(kept[:, None], (windows, levels))

    slot_of = (win_of ^ me) * GCAP + rank
    departures, sums = departures_kernel(
        slab, mirror, near, far_low, far_high, slot_of, win_of, wanted[me], wanted[me ^ opposite], weights, observed,
        used_t, inv_error, kept_rows, low,
    )
    for axis in ("obs", "tm"):
        bits = 1
        while bits < lax.axis_size(axis):
            sums = sums + swap(sums, axis, bits)
            bits *= 2
    mine = lax.dynamic_slice_in_dim(sums, me, 1, 1)
    window_bias = mine[0] / jnp.sqrt(mine[2] + 1.0)
    window_chi = mine[1] / (mine[2] + 1.0)
    return (departures, window_bias, window_chi)


def solution(mesh):
    return jax.shard_map(
        per_device,
        mesh=mesh,
        in_specs=(
            P("tm", "obs", None, None),
            P(("tm", "obs"), None, None),
            P(("tm", "obs"), None, None),
            P(("tm", "obs"), None),
            P(("tm", "obs")),
            P(("tm", "obs")),
            P(("tm", "obs"), None),
            P(),
        ),
        out_specs=(P(("tm", "obs"), None, None), P("tm", None), P("tm", None)),
        check_vma=False,
    )
```

```python
import jax
import jax.numpy as jnp
from jax import lax
from jax.experimental import pallas as pl
from jax.experimental.pallas import tpu as pltpu
from jax.sharding import PartitionSpec as P


GCAP = 4
STEP = 8


ANY = pl.BlockSpec(memory_space=pl.ANY)
SMEM = pl.BlockSpec(memory_space=pltpu.SMEM)


def swap(x, axis, bits):
    size = lax.axis_size(axis)
    return lax.ppermute(x, axis, [(i, i ^ bits) for i in range(size)])


def gather_rows(ids, slab, pieces, first, rows):
    width = slab.shape[2]

    def body(ids_ref, slab_ref, *refs):
        outs, sems = refs[:pieces], refs[pieces]
        copies = []
        for piece in range(pieces):
            for k in range(GCAP):
                copy = pltpu.make_async_copy(
                    slab_ref.at[ids_ref[piece, k], pl.ds(first, rows)],
                    outs[piece].at[k],
                    sems.at[piece * GCAP + k],
                )
                copy.start()
                copies.append(copy)
        for copy in copies:
            copy.wait()

    return pl.pallas_call(
        body,
        in_specs=[SMEM, ANY],
        out_specs=[pl.BlockSpec(memory_space=pltpu.VMEM)] * pieces,
        out_shape=[jax.ShapeDtypeStruct((GCAP, rows, width), slab.dtype)] * pieces,
        scratch_shapes=[pltpu.SemaphoreType.DMA((pieces * GCAP,))],
    )(ids, slab)


def departures_kernel(
    slab, mirror, near, far_low, far_high, slot_of, win_of, own_ids, mirror_ids, weights, observed, used_t, inv_error,
    kept_rows, low,
):
    groups, slots, cells = weights.shape
    levels = observed.shape[2]
    windows = kept_rows.shape[0]
    half = windows // 2
    n_near, n_low, n_high = len(near), len(far_low), len(far_high)
    opposite = windows - 2
    n_sems = 2 * GCAP + n_near + n_low + n_high

    def body(slot_ref, win_ref, own_ref, mir_ref, w_ref, y_ref, u_ref, inv_ref, kept_ref, slab_ref, mirror_ref, *refs):
        near_refs = refs[:n_near]
        low_refs = refs[n_near:n_near + n_low]
        high_refs = refs[n_near + n_low:n_near + n_low + n_high]
        out_ref, sum_ref, x_ref, sems = refs[n_near + n_low + n_high:]
        step = pl.program_id(0)

        @pl.when(step == 0)
        def _():
            copies = []

            def add(src, dst):
                copy = pltpu.make_async_copy(src, dst, sems.at[len(copies)])
                copy.start()
                copies.append(copy)

            for k in range(GCAP):
                add(slab_ref.at[own_ref[k]], x_ref.at[k])
                add(mirror_ref.at[mir_ref[k]], x_ref.at[opposite * GCAP + k, pl.ds(0, low)])
            for j in range(1, half):
                add(near_refs[j - 1], x_ref.at[pl.ds(j * GCAP, GCAP)])
                add(low_refs[j - 1], x_ref.at[pl.ds((j ^ opposite) * GCAP, GCAP), pl.ds(0, low)])
            for j in range(half, windows):
                add(high_refs[j - half], x_ref.at[pl.ds(j * GCAP, GCAP), pl.ds(low, cells - low)])
            sum_ref[0] = jnp.zeros((windows, levels), jnp.float32)
            sum_ref[1] = jnp.zeros((windows, levels), jnp.float32)
            sum_ref[2] = kept_ref[...]
            for copy in copies:
                copy.wait()

        inv = inv_ref[...]
        for i in range(STEP):
            g = step * STEP + i
            x = x_ref[slot_ref[g]]
            hx = jnp.dot(w_ref[i], x, preferred_element_type=jnp.float32)
            dep = u_ref[0, :, i:i + 1] * (y_ref[i].astype(jnp.float32) - hx) * inv
            out_ref[i] = dep.astype(jnp.bfloat16)
            w = win_ref[g]
            sum_ref[0, pl.ds(w, 1), :] += jnp.sum(dep, 0, keepdims=True)
            sum_ref[1, pl.ds(w, 1), :] += jnp.sum(dep * dep, 0, keepdims=True)

    return pl.pallas_call(
        body,
        grid=(groups // STEP,),
        in_specs=[SMEM] * 4
        + [
            pl.BlockSpec((STEP, slots, cells), lambda s: (s, 0, 0)),
            pl.BlockSpec((STEP, slots, levels), lambda s: (s, 0, 0)),
            pl.BlockSpec((1, slots, STEP), lambda s: (s, 0, 0)),
            pl.BlockSpec((1, levels), lambda s: (0, 0)),
            pl.BlockSpec((windows, levels), lambda s: (0, 0)),
        ]
        + [ANY] * (2 + n_near + n_low + n_high),
        out_specs=[
            pl.BlockSpec((STEP, slots, levels), lambda s: (s, 0, 0)),
            pl.BlockSpec((3, windows, levels), lambda s: (0, 0, 0)),
        ],
        out_shape=[
            jax.ShapeDtypeStruct((groups, slots, levels), jnp.bfloat16),
            jax.ShapeDtypeStruct((3, windows, levels), jnp.float32),
        ],
        scratch_shapes=[
            pltpu.VMEM((windows * GCAP, cells, levels), slab.dtype),
            pltpu.SemaphoreType.DMA((n_sems,)),
        ],
    )(
        slot_of, win_of, own_ids, mirror_ids, weights, observed, used_t, inv_error[None, :], kept_rows,
        slab, mirror, *near, *far_low, *far_high,
    )


def body(trajectory, weights, observed, window, block, counts, flags, inv_error):
    groups, slots, cells = weights.shape
    levels = observed.shape[2]
    windows = lax.axis_size("tm")
    half = windows // 2
    opposite = windows - 2
    low = cells * 3 // 8 // 16 * 16
    me = lax.axis_index("tm")
    slab = trajectory[0]

    mirror = swap(slab[:, :low], "tm", opposite)

    win_of = window[:, 0]
    gid = jnp.arange(groups, dtype=jnp.int32)
    rank = jnp.sum(((win_of[:, None] == win_of[None, :]) & (gid[None, :] < gid[:, None])).astype(jnp.int32), 1)
    code = win_of * GCAP + rank
    wanted = jnp.sum(
        jnp.where(code[None, :] == jnp.arange(windows * GCAP, dtype=jnp.int32)[:, None], block[None, :], 0), 1
    ).reshape(windows, GCAP)
    across = wanted.reshape(2, half // 2, 2, GCAP)[::-1, ::-1].reshape(windows, GCAP)
    request = jnp.concatenate([wanted, across], 1)
    asked = lax.all_to_all(request, "tm", split_axis=0, concat_axis=0, tiled=True)
    by_xor = asked[jnp.arange(windows, dtype=jnp.int32) ^ me]

    send_high = gather_rows(by_xor[half:, :GCAP], slab, half, low, cells - low)
    far_high = [swap(send_high[j - half], "tm", j) for j in range(half, windows)]
    send_near = gather_rows(by_xor[1:half, :GCAP], slab, half - 1, 0, cells)
    near = [swap(send_near[j - 1], "tm", j) for j in range(1, half)]
    send_low = gather_rows(by_xor[1:half, GCAP:], mirror, half - 1, 0, low)
    far_low = [swap(send_low[j - 1], "tm", j) for j in range(1, half)]

    slot_ids = lax.broadcasted_iota(jnp.int32, (groups, slots), 1)
    used = jnp.where(slot_ids < counts[:, None], flags, 0).astype(jnp.float32)
    used_t = used.reshape(groups // STEP, STEP, slots).transpose(0, 2, 1)
    member = win_of[None, :] == jnp.arange(windows, dtype=jnp.int32)[:, None]
    kept = jnp.sum(jnp.where(member, jnp.sum(used, 1)[None, :], 0.0), 1)
    kept_rows = jnp.broadcast_to(kept[:, None], (windows, levels))

    slot_of = (win_of ^ me) * GCAP + rank
    departures, sums = departures_kernel(
        slab, mirror, near, far_low, far_high, slot_of, win_of, wanted[me], wanted[me ^ opposite], weights, observed,
        used_t, inv_error, kept_rows, low,
    )
    for axis in ("obs", "tm"):
        bits = 1
        while bits < lax.axis_size(axis):
            sums = sums + swap(sums, axis, bits)
            bits *= 2
    mine = lax.dynamic_slice_in_dim(sums, me, 1, 1)
    window_bias = mine[0] / jnp.sqrt(mine[2] + 1.0)
    window_chi = mine[1] / (mine[2] + 1.0)
    return (departures, window_bias, window_chi)


def solution(mesh):
    return jax.shard_map(
        body,
        mesh=mesh,
        in_specs=(
            P("tm", "obs", None, None),
            P(("tm", "obs"), None, None),
            P(("tm", "obs"), None, None),
            P(("tm", "obs"), None),
            P(("tm", "obs")),
            P(("tm", "obs")),
            P(("tm", "obs"), None),
            P(),
        ),
        out_specs=(P(("tm", "obs"), None, None), P("tm", None), P("tm", None)),
        check_vma=False,
    )
```

```python
import jax
import jax.numpy as jnp
from jax import lax
from jax.experimental import pallas as pl
from jax.experimental.pallas import tpu as pltpu
from jax.sharding import PartitionSpec as P


GCAP = 4
STEP = 8


ANY = pl.BlockSpec(memory_space=pl.ANY)
SMEM = pl.BlockSpec(memory_space=pltpu.SMEM)


def swap(x, axis, bits):
    size = lax.axis_size(axis)
    return lax.ppermute(x, axis, [(i, i ^ bits) for i in range(size)])


def index_kernel(win_of, block, me, windows):
    groups = win_of.shape[0]
    opposite = windows - 2

    def body(win_ref, block_ref, me_ref, request_ref, slot_ref, count_ref):
        def clear(w, carry):
            count_ref[w] = 0
            for k in range(2 * GCAP):
                request_ref[w, k] = 0
            return carry

        lax.fori_loop(0, windows, clear, 0)
        mine = me_ref[0]

        def place(g, carry):
            w = win_ref[g]
            rank = count_ref[w]
            count_ref[w] = rank + 1
            request_ref[w, rank] = block_ref[g]
            request_ref[w ^ opposite, GCAP + rank] = block_ref[g]
            slot_ref[g] = (w ^ mine) * GCAP + rank
            return carry

        lax.fori_loop(0, groups, place, 0)

    return pl.pallas_call(
        body,
        in_specs=[SMEM] * 3,
        out_specs=[SMEM] * 2,
        out_shape=[
            jax.ShapeDtypeStruct((windows, 2 * GCAP), jnp.int32),
            jax.ShapeDtypeStruct((groups,), jnp.int32),
        ],
        scratch_shapes=[pltpu.SMEM((windows,), jnp.int32)],
    )(win_of, block, me)


def gather_rows(asked, me, slab, partners, column, first, rows):
    width = slab.shape[2]
    pieces = len(partners)

    def body(asked_ref, me_ref, slab_ref, *refs):
        outs, stages, arrived, left = refs[:pieces], *refs[pieces:]
        loads, stores = [], []
        for piece, j in enumerate(partners):
            source = j ^ me_ref[0]
            for k in range(GCAP):
                copy = pltpu.make_async_copy(
                    slab_ref.at[asked_ref[source, column + k], pl.ds(first, rows)],
                    stages.at[piece, k],
                    arrived.at[piece * GCAP + k],
                )
                copy.start()
                loads.append(copy)
        for piece in range(pieces):
            for k in range(GCAP):
                loads[piece * GCAP + k].wait()
            copy = pltpu.make_async_copy(stages.at[piece], outs[piece], left.at[piece])
            copy.start()
            stores.append(copy)
        for copy in stores:
            copy.wait()

    return pl.pallas_call(
        body,
        in_specs=[SMEM, SMEM, ANY],
        out_specs=[ANY] * pieces,
        out_shape=[jax.ShapeDtypeStruct((GCAP, rows, width), slab.dtype)] * pieces,
        scratch_shapes=[
            pltpu.VMEM((pieces, GCAP, rows, width), slab.dtype),
            pltpu.SemaphoreType.DMA((pieces * GCAP,)),
            pltpu.SemaphoreType.DMA((pieces,)),
        ],
    )(asked, me, slab)


def departures_kernel(
    slab, mirror, near, far_low, far_high, slot_of, win_of, request, me, weights, observed, used_t, inv_error,
    kept_rows, low,
):
    groups, slots, cells = weights.shape
    levels = observed.shape[2]
    windows = kept_rows.shape[0]
    half = windows // 2
    n_near, n_low, n_high = len(near), len(far_low), len(far_high)
    opposite = windows - 2
    n_sems = 2 * GCAP + n_near + n_low + n_high

    def body(slot_ref, win_ref, request_ref, me_ref, w_ref, y_ref, u_ref, inv_ref, kept_ref, slab_ref, mirror_ref, *refs):
        near_refs = refs[:n_near]
        low_refs = refs[n_near:n_near + n_low]
        high_refs = refs[n_near + n_low:n_near + n_low + n_high]
        out_ref, sum_ref, x_ref, sems = refs[n_near + n_low + n_high:]
        step = pl.program_id(0)

        @pl.when(step == 0)
        def _():
            copies = []

            def add(src, dst):
                copy = pltpu.make_async_copy(src, dst, sems.at[len(copies)])
                copy.start()
                copies.append(copy)

            for k in range(GCAP):
                add(slab_ref.at[request_ref[me_ref[0], k]], x_ref.at[k])
                add(mirror_ref.at[request_ref[me_ref[0], GCAP + k]], x_ref.at[opposite * GCAP + k, pl.ds(0, low)])
            for j in range(1, half):
                add(near_refs[j - 1], x_ref.at[pl.ds(j * GCAP, GCAP)])
                add(low_refs[j - 1], x_ref.at[pl.ds((j ^ opposite) * GCAP, GCAP), pl.ds(0, low)])
            for j in range(half, windows):
                add(high_refs[j - half], x_ref.at[pl.ds(j * GCAP, GCAP), pl.ds(low, cells - low)])
            sum_ref[0] = jnp.zeros((windows, levels), jnp.float32)
            sum_ref[1] = jnp.zeros((windows, levels), jnp.float32)
            sum_ref[2] = kept_ref[...]
            for copy in copies:
                copy.wait()

        inv = inv_ref[...]
        for i in range(STEP):
            g = step * STEP + i
            x = x_ref[slot_ref[g]]
            hx = jnp.dot(w_ref[i], x, preferred_element_type=jnp.float32)
            dep = u_ref[0, :, i:i + 1] * (y_ref[i].astype(jnp.float32) - hx) * inv
            out_ref[i] = dep.astype(jnp.bfloat16)
            w = win_ref[g]
            sum_ref[0, pl.ds(w, 1), :] += jnp.sum(dep, 0, keepdims=True)
            sum_ref[1, pl.ds(w, 1), :] += jnp.sum(dep * dep, 0, keepdims=True)

    return pl.pallas_call(
        body,
        grid=(groups // STEP,),
        in_specs=[SMEM] * 4
        + [
            pl.BlockSpec((STEP, slots, cells), lambda s: (s, 0, 0)),
            pl.BlockSpec((STEP, slots, levels), lambda s: (s, 0, 0)),
            pl.BlockSpec((1, slots, STEP), lambda s: (s, 0, 0)),
            pl.BlockSpec((1, levels), lambda s: (0, 0)),
            pl.BlockSpec((windows, levels), lambda s: (0, 0)),
        ]
        + [ANY] * (2 + n_near + n_low + n_high),
        out_specs=[
            pl.BlockSpec((STEP, slots, levels), lambda s: (s, 0, 0)),
            pl.BlockSpec((3, windows, levels), lambda s: (0, 0, 0)),
        ],
        out_shape=[
            jax.ShapeDtypeStruct((groups, slots, levels), jnp.bfloat16),
            jax.ShapeDtypeStruct((3, windows, levels), jnp.float32),
        ],
        scratch_shapes=[
            pltpu.VMEM((windows * GCAP, cells, levels), slab.dtype),
            pltpu.SemaphoreType.DMA((n_sems,)),
        ],
    )(
        slot_of, win_of, request, me, weights, observed, used_t, inv_error[None, :], kept_rows,
        slab, mirror, *near, *far_low, *far_high,
    )


def body(trajectory, weights, observed, window, block, counts, flags, inv_error):
    groups, slots, cells = weights.shape
    levels = observed.shape[2]
    windows = lax.axis_size("tm")
    half = windows // 2
    opposite = windows - 2
    low = cells * 5 // 8 // 16 * 16
    me = lax.axis_index("tm").reshape(1)
    slab = trajectory[0]

    mirror = swap(slab[:, :low], "tm", opposite)

    win_of = window[:, 0]
    request, slot_of = index_kernel(win_of, block, me, windows)
    asked = lax.all_to_all(request[:, None], "tm", split_axis=0, concat_axis=0, tiled=True)[:, 0]

    far = tuple(range(half, windows))
    close = tuple(range(1, half))
    sent = gather_rows(asked, me, slab, far, 0, low, cells - low)
    far_high = [swap(part, "tm", j) for j, part in zip(far, sent)]
    sent = gather_rows(asked, me, slab, close, 0, 0, cells)
    near = [swap(part, "tm", j) for j, part in zip(close, sent)]
    sent = gather_rows(asked, me, mirror, close, GCAP, 0, low)
    far_low = [swap(part, "tm", j) for j, part in zip(close, sent)]

    slot_ids = lax.broadcasted_iota(jnp.int32, (groups, slots), 1)
    used = jnp.where(slot_ids < counts[:, None], flags, 0).astype(jnp.float32)
    used_t = used.reshape(groups // STEP, STEP, slots).transpose(0, 2, 1)
    member = win_of[None, :] == jnp.arange(windows, dtype=jnp.int32)[:, None]
    kept = jnp.sum(jnp.where(member, jnp.sum(used, 1)[None, :], 0.0), 1)
    kept_rows = jnp.broadcast_to(kept[:, None], (windows, levels))

    departures, sums = departures_kernel(
        slab, mirror, near, far_low, far_high, slot_of, win_of, request, me, weights, observed,
        used_t, inv_error, kept_rows, low,
    )
    for axis in ("obs", "tm"):
        bits = 1
        while bits < lax.axis_size(axis):
            sums = sums + swap(sums, axis, bits)
            bits *= 2
    mine = lax.dynamic_slice_in_dim(sums, me[0], 1, 1)
    window_bias = mine[0] / jnp.sqrt(mine[2] + 1.0)
    window_chi = mine[1] / (mine[2] + 1.0)
    return (departures, window_bias, window_chi)


def solution(mesh):
    return jax.shard_map(
        body,
        mesh=mesh,
        in_specs=(
            P("tm", "obs", None, None),
            P(("tm", "obs"), None, None),
            P(("tm", "obs"), None, None),
            P(("tm", "obs"), None),
            P(("tm", "obs")),
            P(("tm", "obs")),
            P(("tm", "obs"), None),
            P(),
        ),
        out_specs=(P(("tm", "obs"), None, None), P("tm", None), P("tm", None)),
        check_vma=False,
    )
```

```python
import jax
import jax.numpy as jnp
from jax import lax
from jax.experimental import pallas as pl
from jax.experimental.pallas import tpu as pltpu
from jax.sharding import PartitionSpec as P


GCAP = 4
STEP = 8


ANY = pl.BlockSpec(memory_space=pl.ANY)
SMEM = pl.BlockSpec(memory_space=pltpu.SMEM)


def swap(x, axis, bits):
    size = lax.axis_size(axis)
    return lax.ppermute(x, axis, [(i, i ^ bits) for i in range(size)])


def index_kernel(win_of, block, me, windows):
    groups = win_of.shape[0]
    opposite = windows - 2

    def body(win_ref, block_ref, me_ref, request_ref, slot_ref, count_ref):
        def clear(w, carry):
            count_ref[w] = 0
            for k in range(2 * GCAP):
                request_ref[w, k] = 0
            return carry

        lax.fori_loop(0, windows, clear, 0)
        mine = me_ref[0]

        def place(g, carry):
            w = win_ref[g]
            rank = count_ref[w]
            count_ref[w] = rank + 1
            request_ref[w, rank] = block_ref[g]
            request_ref[w ^ opposite, GCAP + rank] = block_ref[g]
            slot_ref[g] = (w ^ mine) * GCAP + rank
            return carry

        lax.fori_loop(0, groups, place, 0)

    return pl.pallas_call(
        body,
        in_specs=[SMEM] * 3,
        out_specs=[SMEM] * 2,
        out_shape=[
            jax.ShapeDtypeStruct((windows, 2 * GCAP), jnp.int32),
            jax.ShapeDtypeStruct((groups,), jnp.int32),
        ],
        scratch_shapes=[pltpu.SMEM((windows,), jnp.int32)],
    )(win_of, block, me)


def gather_rows(asked, me, sources, partners):
    count = len(sources)
    width = sources[0][0].shape[2]
    dtype = sources[0][0].dtype
    pieces = len(partners)
    total = sum(rows for _, _, _, rows in sources)

    def body(asked_ref, me_ref, *refs):
        source_refs, outs = refs[:count], refs[count:count + pieces]
        stages, arrived, left = refs[count + pieces:]
        loads, stores = [], []
        for piece, j in enumerate(partners):
            asker = j ^ me_ref[0]
            for k in range(GCAP):
                at = 0
                for ref, (_, column, first, rows) in zip(source_refs, sources):
                    copy = pltpu.make_async_copy(
                        ref.at[asked_ref[asker, column + k], pl.ds(first, rows)],
                        stages.at[piece, k, pl.ds(at, rows)],
                        arrived.at[len(loads)],
                    )
                    copy.start()
                    loads.append(copy)
                    at += rows
        each = GCAP * count
        for piece in range(pieces):
            for copy in loads[piece * each:(piece + 1) * each]:
                copy.wait()
            copy = pltpu.make_async_copy(stages.at[piece], outs[piece], left.at[piece])
            copy.start()
            stores.append(copy)
        for copy in stores:
            copy.wait()

    return pl.pallas_call(
        body,
        in_specs=[SMEM, SMEM] + [ANY] * count,
        out_specs=[ANY] * pieces,
        out_shape=[jax.ShapeDtypeStruct((GCAP, total, width), dtype)] * pieces,
        scratch_shapes=[
            pltpu.VMEM((pieces, GCAP, total, width), dtype),
            pltpu.SemaphoreType.DMA((pieces * GCAP * count,)),
            pltpu.SemaphoreType.DMA((pieces,)),
        ],
    )(asked, me, *[array for array, _, _, _ in sources])


def departures_kernel(
    slab, mirror, near, far_high, slot_of, win_of, request, me, weights, observed, used_t, inv_error,
    kept, low,
):
    groups, slots, cells = weights.shape
    levels = observed.shape[2]
    windows = kept.shape[0]
    half = windows // 2
    n_near, n_high = len(near), len(far_high)
    opposite = windows - 2
    n_sems = 2 * GCAP + 2 * n_near + n_high

    def body(slot_ref, win_ref, request_ref, me_ref, w_ref, y_ref, u_ref, inv_ref, kept_ref, slab_ref, mirror_ref, *refs):
        near_refs = refs[:n_near]
        high_refs = refs[n_near:n_near + n_high]
        out_ref, sum_ref, x_ref, sems = refs[n_near + n_high:]
        step = pl.program_id(0)

        @pl.when(step == 0)
        def _():
            copies = []

            def add(src, dst):
                copy = pltpu.make_async_copy(src, dst, sems.at[len(copies)])
                copy.start()
                copies.append(copy)

            for k in range(GCAP):
                add(slab_ref.at[request_ref[me_ref[0], k]], x_ref.at[k])
                add(mirror_ref.at[request_ref[me_ref[0], GCAP + k]], x_ref.at[opposite * GCAP + k, pl.ds(0, low)])
            for j in range(1, half):
                add(near_refs[j - 1].at[:, pl.ds(0, cells)], x_ref.at[pl.ds(j * GCAP, GCAP)])
                add(near_refs[j - 1].at[:, pl.ds(cells, low)], x_ref.at[pl.ds((j ^ opposite) * GCAP, GCAP), pl.ds(0, low)])
            for j in range(half, windows):
                add(high_refs[j - half], x_ref.at[pl.ds(j * GCAP, GCAP), pl.ds(low, cells - low)])
            sum_ref[0] = jnp.zeros((windows, levels), jnp.float32)
            sum_ref[1] = jnp.zeros((windows, levels), jnp.float32)
            sum_ref[2] = jnp.broadcast_to(kept_ref[...], (windows, levels))
            for copy in copies:
                copy.wait()

        inv = inv_ref[...]
        for i in range(STEP):
            g = step * STEP + i
            x = x_ref[slot_ref[g]]
            hx = jnp.dot(w_ref[i], x, preferred_element_type=jnp.float32)
            dep = u_ref[0, :, i:i + 1] * (y_ref[i].astype(jnp.float32) - hx) * inv
            out_ref[i] = dep.astype(jnp.bfloat16)
            w = win_ref[g]
            sum_ref[0, pl.ds(w, 1), :] += jnp.sum(dep, 0, keepdims=True)
            sum_ref[1, pl.ds(w, 1), :] += jnp.sum(dep * dep, 0, keepdims=True)

    return pl.pallas_call(
        body,
        grid=(groups // STEP,),
        in_specs=[SMEM] * 4
        + [
            pl.BlockSpec((STEP, slots, cells), lambda s: (s, 0, 0)),
            pl.BlockSpec((STEP, slots, levels), lambda s: (s, 0, 0)),
            pl.BlockSpec((1, slots, STEP), lambda s: (s, 0, 0)),
            pl.BlockSpec((1, levels), lambda s: (0, 0)),
            pl.BlockSpec((windows, 1), lambda s: (0, 0)),
        ]
        + [ANY] * (2 + n_near + n_high),
        out_specs=[
            pl.BlockSpec((STEP, slots, levels), lambda s: (s, 0, 0)),
            pl.BlockSpec((3, windows, levels), lambda s: (0, 0, 0)),
        ],
        out_shape=[
            jax.ShapeDtypeStruct((groups, slots, levels), jnp.bfloat16),
            jax.ShapeDtypeStruct((3, windows, levels), jnp.float32),
        ],
        scratch_shapes=[
            pltpu.VMEM((windows * GCAP, cells, levels), slab.dtype),
            pltpu.SemaphoreType.DMA((n_sems,)),
        ],
    )(
        slot_of, win_of, request, me, weights, observed, used_t, inv_error[None, :], kept,
        slab, mirror, *near, *far_high,
    )


def body(trajectory, weights, observed, window, block, counts, flags, inv_error):
    groups, slots, cells = weights.shape
    windows = lax.axis_size("tm")
    half = windows // 2
    opposite = windows - 2
    low = cells * 3 // 8 // 16 * 16
    me = lax.axis_index("tm").reshape(1)
    slab = trajectory[0]

    mirror = swap(slab[:, :low], "tm", opposite)

    win_of = window[:, 0]
    request, slot_of = index_kernel(win_of, block, me, windows)
    asked = lax.all_to_all(request[:, None], "tm", split_axis=0, concat_axis=0, tiled=True)[:, 0]

    far = tuple(range(half, windows))
    close = tuple(range(1, half))
    sent = gather_rows(asked, me, ((slab, 0, low, cells - low),), far)
    far_high = [swap(part, "tm", j) for j, part in zip(far, sent)]
    sent = gather_rows(asked, me, ((slab, 0, 0, cells), (mirror, GCAP, 0, low)), close)
    near = [swap(part, "tm", j) for j, part in zip(close, sent)]

    slot_ids = lax.broadcasted_iota(jnp.int32, (groups, slots), 1)
    used = jnp.where(slot_ids < counts[:, None], flags, 0).astype(jnp.float32)
    used_t = used.reshape(groups // STEP, STEP, slots).transpose(0, 2, 1)
    member = win_of[None, :] == jnp.arange(windows, dtype=jnp.int32)[:, None]
    kept = jnp.sum(jnp.where(member, jnp.sum(used, 1)[None, :], 0.0), 1, keepdims=True)
    departures, sums = departures_kernel(
        slab, mirror, near, far_high, slot_of, win_of, request, me, weights, observed,
        used_t, inv_error, kept, low,
    )
    for axis in ("obs", "tm"):
        bits = 1
        while bits < lax.axis_size(axis):
            sums = sums + swap(sums, axis, bits)
            bits *= 2
    mine = lax.dynamic_slice_in_dim(sums, me[0], 1, 1)
    window_bias = mine[0] / jnp.sqrt(mine[2] + 1.0)
    window_chi = mine[1] / (mine[2] + 1.0)
    return (departures, window_bias, window_chi)


def solution(mesh):
    return jax.shard_map(
        body,
        mesh=mesh,
        in_specs=(
            P("tm", "obs", None, None),
            P(("tm", "obs"), None, None),
            P(("tm", "obs"), None, None),
            P(("tm", "obs"), None),
            P(("tm", "obs")),
            P(("tm", "obs")),
            P(("tm", "obs"), None),
            P(),
        ),
        out_specs=(P(("tm", "obs"), None, None), P("tm", None), P("tm", None)),
        check_vma=False,
    )
```
